32 devices in a mesh: rep: 1, r: 4 (over z), s: 8 (over x, y, core).
Axes of the slice: x: 2, y: 2, z: 4, core: 2. Of those that a mesh axis runs over, the one named last changes fastest.
Arguments:
- x: bfloat16 [32, 4096, 640], P(('rep', 'r', 's'))
- dy: bfloat16 [32, 4096, 640], P(('rep', 'r', 's'))
- w_gate: bfloat16 [2, 640, 2048], P(None, 's')
- w_up: bfloat16 [2, 640, 2048], P(None, 's')
- w_down: bfloat16 [2, 2048, 640], P(None, 's')
Outputs:
- output 1: bfloat16 [32, 4096, 640], P(('rep', 'r', 's'))
- output 2: bfloat16 [2, 640, 2048], P('rep', 's')
- output 3: bfloat16 [2, 640, 2048], P('rep', 's')
- output 4: bfloat16 [2, 2048, 640], P('rep', 's')
All inputs are finite; a program needn't handle non-finite values.
Results may differ from the reference program's by a relative error of at most 0.018.
Values are sent between devices in bfloat16 or wider.
A program may use at most 2 GiB of HBM per device.

```python
import jax
import jax.numpy as jnp
from jax import lax

SEQUENCES = 32
TOKENS = 4096
D = 640
FF = 2048
LAYERS = 2
NAMES = ("w_gate", "w_up", "w_down")
SHAPES = {"w_gate": (LAYERS, D, FF), "w_up": (LAYERS, D, FF), "w_down": (LAYERS, FF, D)}


def bump(key, n, height):
    away = (jnp.arange(n, dtype=jnp.int32) - jax.random.randint(key, (), 0, n, jnp.int32)) % n
    return jnp.where(away < n // 8, height, 1.0)


def together(key, own, strength):
    shared = jax.random.normal(key, own.shape[1:], jnp.float32)
    return (own + strength * shared) * lax.rsqrt(1 + strength * strength)


def setup_inputs(seed: int = 0, part: int = 0) -> dict:
    kx, kdy, ka, kb, kz, kf, kh, kl, *kw = jax.random.split(jax.random.key(seed), 8 + len(NAMES))
    kx, kdy, ka, kb = (jax.random.fold_in(k, part) for k in (kx, kdy, ka, kb))
    shape = (SEQUENCES, TOKENS, D)
    much_x, much_dy = jax.random.uniform(kz, (2,), jnp.float32, 0.0, 1.0)
    layers = 2.0 ** jax.random.uniform(kl, (LAYERS, 1, 1), jnp.float32, -1.0, 1.0)
    x = together(ka, jax.random.normal(kx, shape, jnp.float32), much_x) * bump(kf, D, 4.0)
    dy = together(kb, jax.random.normal(kdy, shape, jnp.float32), much_dy)
    drawn = {"x": x.astype(jnp.bfloat16), "dy": (dy * (SEQUENCES * TOKENS) ** -0.5).astype(jnp.bfloat16)}
    for key, name in zip(kw, NAMES, strict=True):
        w = jax.random.normal(key, SHAPES[name], jnp.float32) * SHAPES[name][1] ** -0.5
        drawn[name] = (w * {"w_gate": 1.0, "w_up": bump(kh, FF, 4.0), "w_down": layers}[name]).astype(jnp.bfloat16)
    return drawn


def matmul(a, w):
    return jnp.dot(a, w, preferred_element_type=jnp.float32).astype(jnp.bfloat16)


def normed(h):
    wide = h.astype(jnp.float32)
    scale = lax.rsqrt(jnp.mean(wide**2, -1, keepdims=True) + 1e-6)
    return (wide * scale).astype(jnp.bfloat16)


def layer(h, w):
    a = normed(h)
    gate = jnp.dot(a, w["w_gate"], preferred_element_type=jnp.float32)
    up = jnp.dot(a, w["w_up"], preferred_element_type=jnp.float32)
    return h + matmul((jax.nn.silu(gate) * up).astype(jnp.bfloat16), w["w_down"])


def stack(weights, h):
    return lax.scan(lambda h, w: (layer(h, w), None), h, weights)[0]


def reference(x, dy, w_gate, w_up, w_down):
    weights = dict(zip(NAMES, (w_gate, w_up, w_down), strict=True))

    def take(so_far, sequence):
        h, by_y = sequence
        _, back = jax.vjp(stack, weights, h)
        by_weights, by_h = back(by_y)
        return jax.tree.map(lambda total, term: total + term.astype(jnp.float32), so_far, by_weights), by_h

    none_yet = {name: jnp.zeros(w.shape, jnp.float32) for name, w in weights.items()}
    by_weights, by_x = lax.scan(take, none_yet, (x, dy))
    return (by_x, *(by_weights[name].astype(jnp.bfloat16) for name in NAMES))
```

```python
import functools

import jax
import jax.numpy as jnp
from jax import lax
from jax.experimental import pallas as pl
from jax.experimental.pallas import tpu as pltpu
from jax.sharding import PartitionSpec as P

F32, BF16 = jnp.float32, jnp.bfloat16
MESH = pl.DeviceIdType.MESH
VMEM_LIMIT = 66_000_000
EPS = 1e-6


def dot(a, b, dims=((1,), (0,))):
    return lax.dot_general(a, b, (dims, ((), ())), preferred_element_type=F32)


def places():
    me = lax.axis_index("s")
    core, y, x = me % 2, (me // 2) % 2, me // 4
    to_x, to_y = 4 - 8 * x, 2 - 4 * y
    return me, me + 1 - 2 * core, me + to_x, me + to_y, me + to_x + to_y


def greet(peers):
    barrier = pltpu.get_barrier_semaphore()
    for peer in peers:
        pl.semaphore_signal(barrier, inc=1, device_id=peer, device_id_type=MESH)
    pl.semaphore_wait(barrier, len(peers))


def remote(src, dst, send, recv, peer):
    return pltpu.make_async_remote_copy(src_ref=src, dst_ref=dst, send_sem=send, recv_sem=recv, device_id=peer, device_id_type=MESH)


class Fetch:
    def __init__(self, shards, wholes, send, recv, local):
        self.me, self.mate, self.xn, self.yn, self.dn = places()
        self.shards, self.wholes, self.send, self.recv, self.local = shards, wholes, send, recv, local

    def peers(self):
        return [{"s": p} for p in (self.mate, self.xn, self.yn)]

    def half(self, m, which, h):
        whole = self.wholes[m]
        rows, cols = whole.shape[1:]
        if m == 2:
            return whole.at[which, pl.ds(h * (rows // 2), rows // 2), :]
        return whole.at[which, :, pl.ds(h * (cols // 2), cols // 2)]

    def copy(self, m, k):
        sems = self.send.at[m, k], self.recv.at[m, k]
        whole, shard = self.wholes[m], self.shards[m]
        if k < 3:
            return remote(shard, whole.at[self.me], *sems, {"s": (self.mate, self.xn, self.yn)[k]})
        if k == 3:
            return remote(self.half(m, self.xn, 0), self.half(m, self.xn, 0), *sems, {"s": self.yn})
        if k == 4:
            return remote(self.half(m, self.yn, 1), self.half(m, self.yn, 1), *sems, {"s": self.xn})
        which = (self.xn, self.yn, self.dn)[k - 5]
        return remote(whole.at[which], whole.at[which], *sems, {"s": self.mate})

    def own(self, m):
        return pltpu.make_async_copy(self.shards[m], self.wholes[m].at[self.me], self.local.at[m])

    def begin(self):
        for m in range(3):
            for k in (1, 2, 0):
                self.copy(m, k).start()
            self.own(m).start()

    def forward(self):
        for m in range(3):
            self.copy(m, 1).wait_recv()
            self.copy(m, 2).wait_recv()
            for k in (3, 4, 5, 6):
                self.copy(m, k).start()

    def finish(self):
        for m in range(3):
            self.copy(m, 3).wait_recv()
            self.copy(m, 4).wait_recv()
            self.copy(m, 7).start()
        for m in range(3):
            for k in (0, 5, 6, 7):
                self.copy(m, k).wait_recv()
            for k in range(8):
                self.copy(m, k).wait_send()
            self.own(m).wait()


FETCH_SCRATCH = [pltpu.SemaphoreType.DMA((3, 8)), pltpu.SemaphoreType.DMA((3, 8)), pltpu.SemaphoreType.DMA((3,))]


def whole_shapes(shards):
    return [jax.ShapeDtypeStruct((8, *w.shape), w.dtype) for w in shards]


def flat(wholes):
    return [w.reshape(-1, w.shape[-1]) for w in wholes]


def fetch_kernel(*refs):
    fetch = Fetch(refs[:3], refs[3:6], *refs[6:])
    greet(fetch.peers())
    fetch.begin()
    fetch.forward()
    fetch.finish()


def fetched(shards, collective_id):
    sent = sum(3 * w.size * 2 for w in shards)
    return flat(
        pl.pallas_call(
            fetch_kernel,
            out_shape=whole_shapes(shards),
            in_specs=[pl.BlockSpec(memory_space=pltpu.VMEM)] * 3,
            out_specs=[pl.BlockSpec(memory_space=pl.ANY)] * 3,
            scratch_shapes=FETCH_SCRATCH,
            compiler_params=pltpu.CompilerParams(collective_id=collective_id, has_side_effects=True, vmem_limit_bytes=VMEM_LIMIT),
            cost_estimate=pl.CostEstimate(flops=0, bytes_accessed=sent, transcendentals=0),
            name="fetch",
        )(*shards)
    )


def normed(h):
    wide = h.astype(F32)
    scale = lax.rsqrt(jnp.mean(wide * wide, -1, keepdims=True) + EPS)
    return wide, scale, (wide * scale).astype(BF16)


def forward_kernel(steps, chunk, x, wg, wu, wd, sg, su, sd, out, og, ou, od, hidden, send, recv, local):
    step = pl.program_id(0)
    fetch = Fetch((sg, su, sd), (og, ou, od), send, recv, local)

    @pl.when(step == 0)
    def _():
        greet(fetch.peers())
        fetch.begin()

    @pl.when(step == steps * 5 // 8)
    def _():
        fetch.forward()

    h = x[...]
    _, _, a = normed(h)
    for j in range(wg.shape[1] // chunk):
        cut = pl.ds(j * chunk, chunk)
        gate, up = dot(a, wg[:, cut]), dot(a, wu[:, cut])
        hidden[:, cut] = (gate * lax.logistic(gate) * up).astype(BF16)
    down = dot(hidden[...], wd[...]).astype(BF16)
    out[...] = (h.astype(F32) + down.astype(F32)).astype(BF16)

    @pl.when(step == steps - 1)
    def _():
        fetch.finish()


def constant(shape):
    return pl.BlockSpec(shape, lambda i: (0,) * len(shape), pipeline_mode=pl.Buffered(1))


def forward(x, weights, next_shards, collective_id, tile=512, chunk=512):
    tokens, d = x.shape
    ff = weights[0].shape[1]
    steps = tokens // tile
    rows = pl.BlockSpec((tile, d), lambda i: (i, 0))
    out, *wholes = pl.pallas_call(
        functools.partial(forward_kernel, steps, chunk),
        grid=(steps,),
        out_shape=[jax.ShapeDtypeStruct(x.shape, BF16), *whole_shapes(next_shards)],
        in_specs=[rows, *[constant(w.shape) for w in weights], *[constant(w.shape) for w in next_shards]],
        out_specs=[rows, *[pl.BlockSpec(memory_space=pl.ANY)] * 3],
        scratch_shapes=[pltpu.VMEM((tile, ff), BF16), *FETCH_SCRATCH],
        compiler_params=pltpu.CompilerParams(
            collective_id=collective_id, has_side_effects=True, vmem_limit_bytes=VMEM_LIMIT, dimension_semantics=("arbitrary",)
        ),
        cost_estimate=pl.CostEstimate(flops=6 * tokens * d * ff, bytes_accessed=4 * tokens * d, transcendentals=0),
        name="forward",
    )(x, *weights, *next_shards)
    return out, flat(wholes)


def act_kernel(steps, chunk, h, dy, wg, wu, wd, by_gu, a_t, by_down, total):
    step = pl.program_id(0)

    @pl.when(step == 0)
    def _():
        total[...] = jnp.zeros_like(total)

    _, _, a = normed(h[...])
    g = dy[...]
    a_t[...] = a.T
    g_t = g.T
    for j in range(wg.shape[1] // chunk):
        cut = pl.ds(j * chunk, chunk)
        gate, up = dot(a, wg[:, cut]), dot(a, wu[:, cut])
        by_hidden = dot(g, wd[cut, :], ((1,), (1,))).astype(BF16).astype(F32)
        share = lax.logistic(gate)
        silu = gate * share
        by_gu[0, :, cut] = (by_hidden * up * (share + silu * (1.0 - share))).astype(BF16)
        by_gu[1, :, cut] = (by_hidden * silu).astype(BF16)
        total[:, cut] += dot(g_t, (silu * up).astype(BF16))

    @pl.when(step == steps - 1)
    def _():
        n = by_down.shape[1]
        for s in range(by_down.shape[0]):
            by_down[s] = total[:, s * n : (s + 1) * n].T.astype(BF16)


def act(h, dy, weights, tile=512, chunk=512):
    tokens, d = h.shape
    ff = weights[0].shape[1]
    steps = tokens // tile
    rows = pl.BlockSpec((tile, d), lambda i: (i, 0))
    return pl.pallas_call(
        functools.partial(act_kernel, steps, chunk),
        grid=(steps,),
        out_shape=[
            jax.ShapeDtypeStruct((2, tokens, ff), BF16),
            jax.ShapeDtypeStruct((d, tokens), BF16),
            jax.ShapeDtypeStruct((8, ff // 8, d), BF16),
        ],
        in_specs=[rows, rows, *[constant(w.shape) for w in weights]],
        out_specs=[
            pl.BlockSpec((2, tile, ff), lambda i: (0, i, 0)),
            pl.BlockSpec((d, tile), lambda i: (0, i)),
            pl.BlockSpec((8, ff // 8, d), lambda i: (0, 0, 0)),
        ],
        scratch_shapes=[pltpu.VMEM((d, ff), F32)],
        compiler_params=pltpu.CompilerParams(vmem_limit_bytes=VMEM_LIMIT, dimension_semantics=("arbitrary",)),
        cost_estimate=pl.CostEstimate(flops=8 * tokens * d * ff, bytes_accessed=8 * tokens * ff, transcendentals=0),
        name="act",
    )(h, dy, *weights)


class Sum:
    def __init__(self, m, term, got0, got1, own, parts, got2, done, sems):
        self.m, self.term, self.got0, self.got1, self.own, self.parts, self.got2, self.done = m, term, got0, got1, own, parts, got2, done
        self.sems = sems
        self.me, self.mate, xn, yn, dn = places()
        self.near = (xn, yn, dn)
        self.z = lax.axis_index("r")
        self.core, self.chip = self.me % 2, self.me // 2

    def copy(self, k):
        sems = self.sems[0].at[self.m, k], self.sems[1].at[self.m, k]
        if k < 4:
            return remote(self.term.at[2 * k + 1 - self.core], self.got0.at[k], *sems, {"s": self.mate})
        if k < 7:
            to = self.near[k - 4]
            return remote(self.got0.at[to // 2], self.got1.at[k - 4], *sems, {"s": to})
        if k < 10:
            z = (self.z + k - 6) % 4
            return remote(self.parts.at[z], self.got2.at[k - 7], *sems, {"r": z})
        z = (self.z + k - 9) % 4
        return remote(self.done.at[self.z], self.done.at[self.z], *sems, {"r": z})

    def start(self, ks):
        for k in ks:
            self.copy(k).start()

    def wait(self, ks):
        for k in ks:
            self.copy(k).wait()

    def pair(self):
        self.start(range(4))

    def chips(self):
        self.wait(range(4))
        for k, to in enumerate(self.near):
            chip = to // 2
            self.got0[chip] = (self.term[2 * chip + self.core].astype(F32) + self.got0[chip].astype(F32)).astype(BF16)
            self.copy(4 + k).start()
        self.own[...] = self.term[self.me].astype(F32) + self.got0[self.chip].astype(F32)

    def groups(self):
        self.wait(range(4, 7))
        whole = self.own[...] + self.got1[0].astype(F32) + self.got1[1].astype(F32) + self.got1[2].astype(F32)
        self.own[...] = whole
        n = self.parts.shape
        for q in range(4):
            self.parts[q] = (whole[:, q * n[2] : (q + 1) * n[2]] if self.m else whole[q * n[1] : (q + 1) * n[1]]).astype(BF16)
        self.start(range(7, 10))

    def share(self):
        self.wait(range(7, 10))
        n = self.parts.shape
        if self.m:
            mine = self.own[:, pl.ds(pl.multiple_of(self.z * n[2], 128), n[2])]
        else:
            mine = self.own[pl.ds(pl.multiple_of(self.z * n[1], 8), n[1]), :]
        for k in range(3):
            mine = mine + self.got2[k].astype(F32)
        self.done[self.z] = mine.astype(BF16)
        self.start(range(10, 13))

    def end(self, out):
        self.wait(range(10, 13))
        n = self.parts.shape
        for q in range(4):
            if self.m:
                out[:, q * n[2] : (q + 1) * n[2]] = self.done[q]
            else:
                out[q * n[1] : (q + 1) * n[1], :] = self.done[q]


def sum_scratch(m, rows, cols):
    part = (4, rows, cols // 4) if m else (4, rows // 4, cols)
    return [
        pltpu.VMEM((4, rows, cols), BF16),
        pltpu.VMEM((3, rows, cols), BF16),
        pltpu.VMEM((rows, cols), F32),
        pltpu.VMEM(part, BF16),
        pltpu.VMEM((3, *part[1:]), BF16),
        pltpu.VMEM(part, BF16),
    ]


def tail_kernel(nw, nt, a_t, wide_gu, by_gu, wg, wu, h, dy, by_down, by_h, out_g, out_u, out_d, term_g, term_u, *scratch):
    step = pl.program_id(0)
    sems = scratch[-2:]
    down = Sum(0, by_down, *scratch[0:6], sems)
    gate = Sum(1, term_g, *scratch[6:12], sems)
    up = Sum(2, term_u, *scratch[12:18], sems)

    def at(n):
        return lambda f: pl.when(step == n)(f)

    @at(0)
    def _():
        me, mate, *near = places()
        z = lax.axis_index("r")
        greet([{"s": p} for p in (mate, *near)] + [{"r": (z + k) % 4} for k in (1, 2, 3)])
        down.pair()

    at(2)(down.chips)
    at(nw)(gate.pair)
    at(nw + nw // 2)(gate.chips)
    at(2 * nw)(up.pair)

    @at(2 * nw + 1)
    def _():
        down.groups()

    at(2 * nw + 2)(up.chips)

    @at(2 * nw + nt // 2)
    def _():
        down.share()
        gate.groups()

    def weight(term, n):
        width = wide_gu.shape[2]
        got = dot(a_t[...], wide_gu[0]).astype(BF16)
        rows = term.shape[1]
        for s in range(8):
            term[s, :, pl.ds(pl.multiple_of(n * width, 128), width)] = got[s * rows : (s + 1) * rows]

    @pl.when(step < nw)
    def _():
        weight(term_g, step)

    @pl.when((step >= nw) & (step < 2 * nw))
    def _():
        weight(term_u, step - nw)

    @pl.when(step >= 2 * nw)
    def _():
        by_a = dot(by_gu[0], wg[...], ((1,), (1,))) + dot(by_gu[1], wu[...], ((1,), (1,)))
        by_a = by_a.astype(BF16).astype(F32)
        wide = h[...].astype(F32)
        scale = lax.rsqrt(jnp.mean(wide * wide, -1, keepdims=True) + EPS)
        pull = jnp.mean(by_a * wide, -1, keepdims=True) * scale * scale * scale
        by_h[...] = (dy[...].astype(F32) + (by_a * scale - wide * pull).astype(BF16).astype(F32)).astype(BF16)

    @at(2 * nw + nt - 1)
    def _():
        gate.share()
        up.groups()
        down.end(out_d)
        up.share()
        gate.end(out_g)
        up.end(out_u)


def tail(a_t, by_gu, wg, wu, h, dy, by_down, collective_id, width=512, tile=512):
    d, tokens = a_t.shape
    ff = wg.shape[1]
    nw, nt = ff // width, tokens // tile
    place = lambda i: jnp.maximum(i - 2 * nw, 0)
    rows = pl.BlockSpec((tile, d), lambda i: (place(i), 0))
    last = 2 * nw - 1
    gate_block, down_block = (d // 8, ff), (ff // 8, d)
    return pl.pallas_call(
        functools.partial(tail_kernel, nw, nt),
        grid=(2 * nw + nt,),
        out_shape=[
            jax.ShapeDtypeStruct((tokens, d), BF16),
            jax.ShapeDtypeStruct(gate_block, BF16),
            jax.ShapeDtypeStruct(gate_block, BF16),
            jax.ShapeDtypeStruct(down_block, BF16),
        ],
        in_specs=[
            constant(a_t.shape),
            pl.BlockSpec((1, tokens, width), lambda i: (jnp.minimum(i, last) // nw, 0, jnp.minimum(i, last) % nw)),
            pl.BlockSpec((2, tile, ff), lambda i: (0, place(i), 0)),
            constant(wg.shape),
            constant(wu.shape),
            rows,
            rows,
            constant(by_down.shape),
        ],
        out_specs=[
            rows,
            pl.BlockSpec(gate_block, lambda i: (0, 0)),
            pl.BlockSpec(gate_block, lambda i: (0, 0)),
            pl.BlockSpec(down_block, lambda i: (0, 0)),
        ],
        scratch_shapes=[
            pltpu.VMEM((8, *gate_block), BF16),
            pltpu.VMEM((8, *gate_block), BF16),
            *sum_scratch(0, *down_block),
            *sum_scratch(1, *gate_block),
            *sum_scratch(2, *gate_block),
            pltpu.SemaphoreType.DMA((3, 13)),
            pltpu.SemaphoreType.DMA((3, 13)),
        ],
        compiler_params=pltpu.CompilerParams(
            collective_id=collective_id, has_side_effects=True, vmem_limit_bytes=VMEM_LIMIT, dimension_semantics=("arbitrary",)
        ),
        cost_estimate=pl.CostEstimate(flops=8 * tokens * d * ff, bytes_accessed=8 * tokens * ff, transcendentals=0),
        name="tail",
    )(a_t, by_gu, by_gu, wg, wu, h, dy, by_down)


def solution(mesh):
    def step(x, dy, *shards):
        layers = shards[0].shape[0]
        shard = [[w[n] for w in shards] for n in range(layers)]
        weights, h, inputs = [fetched(shard[0], 0)], x[0], [x[0]]
        for n in range(layers - 1):
            h, following = forward(h, weights[n], shard[n + 1], 1 + n)
            inputs.append(h)
            weights.append(following)
        by_h, mine = dy[0], [None] * layers
        for n in reversed(range(layers)):
            by_gu, a_t, by_down = act(inputs[n], by_h, weights[n])
            by_h, *mine[n] = tail(a_t, by_gu, *weights[n][:2], inputs[n], by_h, by_down, layers + n)
        return (by_h[None], *(jnp.stack([mine[n][i] for n in range(layers)]) for i in range(3)))

    states, cut = P(("rep", "r", "s"), None, None), P(None, "s", None)
    return jax.shard_map(
        step,
        mesh=mesh,
        in_specs=(states, states) + (cut,) * 3,
        out_specs=(states,) + (P("rep", "s", None),) * 3,
        check_vma=False,
    )
```

```python
import functools

import jax
import jax.numpy as jnp
from jax import lax
from jax.experimental import pallas as pl
from jax.experimental.pallas import tpu as pltpu
from jax.sharding import PartitionSpec as P

F32, BF16 = jnp.float32, jnp.bfloat16
MESH = pl.DeviceIdType.MESH
VMEM_LIMIT = 66_000_000
EPS = 1e-6


def dot(a, b, dims=((1,), (0,))):
    return lax.dot_general(a, b, (dims, ((), ())), preferred_element_type=F32)


def places():
    me = lax.axis_index("s")
    core, y, x = me % 2, (me // 2) % 2, me // 4
    to_x, to_y = 4 - 8 * x, 2 - 4 * y
    return me, me + 1 - 2 * core, me + to_x, me + to_y, me + to_x + to_y


def all_peers():
    _, mate, *near = places()
    z = lax.axis_index("r")
    return [{"s": p} for p in (mate, *near)] + [{"r": (z + k) % 4} for k in (1, 2, 3)]


def greet(peers):
    barrier = pltpu.get_barrier_semaphore()
    for peer in peers:
        pl.semaphore_signal(barrier, inc=1, device_id=peer, device_id_type=MESH)
    pl.semaphore_wait(barrier, len(peers))


def remote(src, dst, send, recv, peer):
    return pltpu.make_async_remote_copy(src_ref=src, dst_ref=dst, send_sem=send, recv_sem=recv, device_id=peer, device_id_type=MESH)


class Piece:
    def __init__(self, block, at, half, send, recv):
        self.me, self.mate, self.xn, self.yn, self.dn = places()
        self.block, self.at, self.half, self.send, self.recv = block, at, half, send, recv

    def copy(self, k):
        sems = self.send.at[k], self.recv.at[k]
        if k < 3:
            return remote(self.block, self.at(self.me), *sems, {"s": (self.mate, self.xn, self.yn)[k]})
        if k == 3:
            return remote(self.half(self.xn, 0), self.half(self.xn, 0), *sems, {"s": self.yn})
        if k == 4:
            return remote(self.half(self.yn, 1), self.half(self.yn, 1), *sems, {"s": self.xn})
        which = (self.xn, self.yn, self.dn)[k - 5]
        return remote(self.at(which), self.at(which), *sems, {"s": self.mate})

    def begin(self):
        for k in (1, 2, 0):
            self.copy(k).start()

    def forward(self):
        self.copy(1).wait_recv()
        self.copy(2).wait_recv()
        for k in (3, 4, 5, 6):
            self.copy(k).start()

    def relay(self):
        self.copy(3).wait_recv()
        self.copy(4).wait_recv()
        self.copy(7).start()

    def settle(self):
        for k in (0, 5, 6, 7):
            self.copy(k).wait_recv()

    def drain(self):
        for k in range(8):
            self.copy(k).wait_send()


def by_columns(block, whole, first, count, *sems):
    cut = lambda slot, start, n: whole.at[slot, :, pl.ds(start, n)]
    return Piece(
        block.at[0, :, pl.ds(first, count)],
        lambda slot: cut(slot, first, count),
        lambda slot, h: cut(slot, first + h * (count // 2), count // 2),
        *sems,
    )


def by_rows(block, whole, *sems):
    n = whole.shape[1] // 2
    return Piece(block.at[0], lambda slot: whole.at[slot], lambda slot, h: whole.at[slot, pl.ds(h * n, n), :], *sems)


def normed(h):
    wide = h.astype(F32)
    scale = lax.rsqrt(jnp.mean(wide * wide, -1, keepdims=True) + EPS)
    return wide, scale, (wide * scale).astype(BF16)


def forward_kernel(nt, nc, x, sg, su, sd, ng, nu, nd, out, og, ou, od, pg, pu, pd, wg, wu, wd, a, hidden, send, recv, local):
    step = pl.program_id(0)
    d, ff = wg.shape[0] * wg.shape[1], wg.shape[2]
    tile, chunk = x.shape[0], ff // nc
    me = lax.axis_index("s")
    sems = lambda n: (send.at[n], recv.at[n])
    c = [
        [by_columns(shard, whole, k * chunk, chunk, *sems(2 * k + n)) for n, (shard, whole) in enumerate([(sg, wg), (su, wu)])]
        for k in range(nc)
    ]
    down = [by_rows(sd, wd, *sems(2 * nc))]
    g1 = [by_columns(ng, pg, 0, ff, *sems(2 * nc + 1))]
    u1 = [by_columns(nu, pu, 0, ff, *sems(2 * nc + 2))]
    d1 = [by_rows(nd, pd, *sems(2 * nc + 3))]
    keep = [pltpu.make_async_copy(p.at[0], q.at[me], local.at[n]) for n, (p, q) in enumerate([(ng, pg), (nu, pu), (nd, pd)])]
    save = [pltpu.make_async_copy(p, q, local.at[3 + n]) for n, (p, q) in enumerate([(wg, og), (wu, ou), (wd, od)])]

    def do(*acts):
        for name, pieces in acts:
            for piece in pieces:
                getattr(piece, name)()

    def first():
        mate, xn, yn = places()[1:4]
        greet([{"s": p} for p in (mate, xn, yn)])
        do(("begin", c[0]), ("begin", c[1]))
        for shard, whole in ((sg, wg), (su, wu), (sd, wd)):
            whole[me] = shard[0]
        for copy in keep:
            copy.start()
        do(("forward", c[0]), ("begin", c[2]), ("relay", c[0]), ("settle", c[0]))

    def all_here():
        do(("settle", down))
        for copy in save:
            copy.start()

    plan = {
        0: first,
        1: lambda: do(("forward", c[1]), ("begin", c[3])),
        3: lambda: do(("relay", c[1]), ("forward", c[2]), ("begin", down)),
        4: lambda: do(("settle", c[1])),
        5: lambda: do(("forward", c[3]), ("begin", g1)),
        6: lambda: do(("relay", c[2])),
        8: lambda: do(("settle", c[2])),
        9: lambda: do(("forward", down), ("begin", u1)),
        10: lambda: do(("relay", c[3])),
        12: lambda: do(("settle", c[3])),
        13: lambda: do(("forward", g1), ("begin", d1)),
        14: lambda: do(("relay", down)),
        16: all_here,
        17: lambda: do(("forward", u1)),
        18: lambda: do(("relay", g1)),
    }
    for n, f in plan.items():
        pl.when(step == n)(f)

    @pl.when(step < nt)
    def _():
        a[step] = normed(x[...])[2]

    @pl.when(step < nt * nc)
    def _():
        cut = pl.ds(pl.multiple_of(step // nt * chunk, chunk), chunk)
        here = a[step % nt]
        gate = dot(here, wg[:, :, cut].reshape(d, chunk))
        up = dot(here, wu[:, :, cut].reshape(d, chunk))
        hidden[step % nt, :, cut] = (gate * lax.logistic(gate) * up).astype(BF16)

    @pl.when(step >= nt * nc)
    def _():
        below = dot(hidden[step - nt * nc], wd[...].reshape(ff, d)).astype(BF16)
        out[...] = (x[...].astype(F32) + below.astype(F32)).astype(BF16)

    @pl.when(step == nt * nc + nt - 1)
    def _():
        do(("forward", d1), ("relay", u1), ("relay", d1), ("settle", g1), ("settle", u1), ("settle", d1))
        for pieces in (*c, down, g1, u1, d1):
            do(("drain", pieces))
        for copy in (*keep, *save):
            copy.wait()


def constant(shape):
    return pl.BlockSpec(shape, lambda i: (0,) * len(shape), pipeline_mode=pl.Buffered(1))


def forward(x, shards, collective_id, nt=4, nc=4):
    tokens, d = x.shape
    ff = shards[0].shape[2]
    tile = tokens // nt
    wholes = [(8, *w.shape[1:]) for w in shards]
    spot = lambda i: jnp.where(i < nt, i, jnp.where(i < nt * nc, nt - 1, i - nt * nc))
    layer = lambda w, n: pl.BlockSpec((1, *w.shape[1:]), lambda i: (n, 0, 0), pipeline_mode=pl.Buffered(1))
    out, *got = pl.pallas_call(
        functools.partial(forward_kernel, nt, nc),
        grid=(nt * nc + nt,),
        out_shape=[jax.ShapeDtypeStruct(x.shape, BF16), *[jax.ShapeDtypeStruct(w, BF16) for w in wholes * 2]],
        in_specs=[pl.BlockSpec((tile, d), lambda i: (spot(i), 0)), *[layer(w, n) for n in range(2) for w in shards]],
        out_specs=[pl.BlockSpec((tile, d), lambda i: (jnp.maximum(i - nt * nc, 0), 0)), *[pl.BlockSpec(memory_space=pl.ANY)] * 6],
        scratch_shapes=[
            *[pltpu.VMEM(w, BF16) for w in wholes],
            pltpu.VMEM((nt, tile, d), BF16),
            pltpu.VMEM((nt, tile, ff), BF16),
            pltpu.SemaphoreType.DMA((2 * nc + 4, 8)),
            pltpu.SemaphoreType.DMA((2 * nc + 4, 8)),
            pltpu.SemaphoreType.DMA((6,)),
        ],
        compiler_params=pltpu.CompilerParams(
            collective_id=collective_id, has_side_effects=True, vmem_limit_bytes=VMEM_LIMIT, dimension_semantics=("arbitrary",)
        ),
        cost_estimate=pl.CostEstimate(flops=6 * tokens * d * ff, bytes_accessed=4 * tokens * d, transcendentals=0),
        name="forward",
    )(x, *shards, *shards)
    got = [w.reshape(-1, w.shape[-1]) for w in got]
    return out, [got[:3], got[3:]]


def act_kernel(steps, chunk, sums, h, dy, wg, wu, wd, *refs):
    step = pl.program_id(0)
    if sums:
        far_g, far_u, by_gu, a_t, by_down, out_g, out_u, total, *scratch, term_g, term_u, local = refs
        loads = [pltpu.make_async_copy(a, b, local.at[n]) for n, (a, b) in enumerate([(far_g, term_g), (far_u, term_u)])]
        gate_sum = Sum(1, term_g, *scratch[:6], scratch[-2:])
        up_sum = Sum(2, term_u, *scratch[6:12], scratch[-2:])

        def begin():
            for load in loads:
                load.start()
            greet(all_peers())
            gate_sum.pair(far_g)
            up_sum.pair(far_u)

        def second():
            for load in loads:
                load.wait()
            gate_sum.chips(far_g)
            up_sum.chips(far_u)

        plan = [(0, begin), (1, second), (3, gate_sum.groups), (4, gate_sum.share), (5, up_sum.groups), (6, up_sum.share)]
        for n, f in plan:
            pl.when(step == steps * n // 8)(f)
    else:
        by_gu, a_t, by_down, total = refs

    @pl.when(step == 0)
    def _():
        total[...] = jnp.zeros_like(total)

    _, _, a = normed(h[...])
    g = dy[...]
    a_t[...] = a.T
    g_t = g.T
    for j in range(wg.shape[1] // chunk):
        cut = pl.ds(j * chunk, chunk)
        gate, up = dot(a, wg[:, cut]), dot(a, wu[:, cut])
        by_hidden = dot(g, wd[cut, :], ((1,), (1,))).astype(BF16).astype(F32)
        share = lax.logistic(gate)
        silu = gate * share
        by_gu[0, :, cut] = (by_hidden * up * (share + silu * (1.0 - share))).astype(BF16)
        by_gu[1, :, cut] = (by_hidden * silu).astype(BF16)
        total[:, cut] += dot(g_t, (silu * up).astype(BF16))

    @pl.when(step == steps - 1)
    def _():
        n = by_down.shape[1]
        for s in range(by_down.shape[0]):
            by_down[s] = total[:, s * n : (s + 1) * n].T.astype(BF16)
        if sums:
            gate_sum.end(out_g)
            up_sum.end(out_u)


def act(h, dy, weights, terms=(), collective_id=None, tile=512, chunk=256):
    tokens, d = h.shape
    ff = weights[0].shape[1]
    steps = tokens // tile
    rows = pl.BlockSpec((tile, d), lambda i: (i, 0))
    block = (d // 8, ff)
    scratch, extra = [], {}
    if terms:
        scratch = [*sum_scratch(1, *block), *sum_scratch(2, *block), pltpu.SemaphoreType.DMA((3, 13)), pltpu.SemaphoreType.DMA((3, 13))]
        scratch += [pltpu.VMEM(w.shape, BF16) for w in terms] + [pltpu.SemaphoreType.DMA((2,))]
        extra = dict(collective_id=collective_id, has_side_effects=True)
    return pl.pallas_call(
        functools.partial(act_kernel, steps, chunk, bool(terms)),
        grid=(steps,),
        out_shape=[
            jax.ShapeDtypeStruct((2, tokens, ff), BF16),
            jax.ShapeDtypeStruct((d, tokens), BF16),
            jax.ShapeDtypeStruct((8, ff // 8, d), BF16),
            *[jax.ShapeDtypeStruct(block, BF16) for _ in terms],
        ],
        in_specs=[rows, rows, *[constant(w.shape) for w in weights], *[pl.BlockSpec(memory_space=pl.ANY) for _ in terms]],
        out_specs=[
            pl.BlockSpec((2, tile, ff), lambda i: (0, i, 0)),
            pl.BlockSpec((d, tile), lambda i: (0, i)),
            pl.BlockSpec((8, ff // 8, d), lambda i: (0, 0, 0)),
            *[pl.BlockSpec(block, lambda i: (0, 0)) for _ in terms],
        ],
        scratch_shapes=[pltpu.VMEM((d, ff), F32), *scratch],
        compiler_params=pltpu.CompilerParams(vmem_limit_bytes=VMEM_LIMIT, dimension_semantics=("arbitrary",), **extra),
        cost_estimate=pl.CostEstimate(flops=8 * tokens * d * ff, bytes_accessed=8 * tokens * ff, transcendentals=0),
        name="act",
    )(h, dy, *weights, *terms)


class Sum:
    def __init__(self, m, term, got0, got1, own, parts, got2, done, sems):
        self.m, self.term, self.got0, self.got1, self.own, self.parts, self.got2, self.done = m, term, got0, got1, own, parts, got2, done
        self.sems = sems
        self.me, self.mate, xn, yn, dn = places()
        self.near = (xn, yn, dn)
        self.z = lax.axis_index("r")
        self.core, self.chip = self.me % 2, self.me // 2

    def copy(self, k, term=None):
        sems = self.sems[0].at[self.m, k], self.sems[1].at[self.m, k]
        if k < 4:
            return remote((self.term if term is None else term).at[2 * k + 1 - self.core], self.got0.at[k], *sems, {"s": self.mate})
        if k < 7:
            to = self.near[k - 4]
            return remote(self.got0.at[to // 2], self.got1.at[k - 4], *sems, {"s": to})
        if k < 10:
            z = (self.z + k - 6) % 4
            return remote(self.parts.at[z], self.got2.at[k - 7], *sems, {"r": z})
        z = (self.z + k - 9) % 4
        return remote(self.done.at[self.z], self.done.at[self.z], *sems, {"r": z})

    def start(self, ks):
        for k in ks:
            self.copy(k).start()

    def wait(self, ks):
        for k in ks:
            self.copy(k).wait()

    def pair(self, term=None):
        for k in range(4):
            self.copy(k, term).start()

    def chips(self, term=None):
        for k in range(4):
            self.copy(k, term).wait()
        for k, to in enumerate(self.near):
            chip = to // 2
            self.got0[chip] = (self.term[2 * chip + self.core].astype(F32) + self.got0[chip].astype(F32)).astype(BF16)
            self.copy(4 + k).start()
        self.own[...] = self.term[self.me].astype(F32) + self.got0[self.chip].astype(F32)

    def groups(self):
        self.wait(range(4, 7))
        whole = self.own[...] + self.got1[0].astype(F32) + self.got1[1].astype(F32) + self.got1[2].astype(F32)
        self.own[...] = whole
        n = self.parts.shape
        for q in range(4):
            self.parts[q] = (whole[:, q * n[2] : (q + 1) * n[2]] if self.m else whole[q * n[1] : (q + 1) * n[1]]).astype(BF16)
        self.start(range(7, 10))

    def share(self):
        self.wait(range(7, 10))
        n = self.parts.shape
        if self.m:
            mine = self.own[:, pl.ds(pl.multiple_of(self.z * n[2], 128), n[2])]
        else:
            mine = self.own[pl.ds(pl.multiple_of(self.z * n[1], 8), n[1]), :]
        for k in range(3):
            mine = mine + self.got2[k].astype(F32)
        self.done[self.z] = mine.astype(BF16)
        self.start(range(10, 13))

    def end(self, out):
        self.wait(range(10, 13))
        n = self.parts.shape
        for q in range(4):
            if self.m:
                out[:, q * n[2] : (q + 1) * n[2]] = self.done[q]
            else:
                out[q * n[1] : (q + 1) * n[1], :] = self.done[q]


def sum_scratch(m, rows, cols):
    part = (4, rows, cols // 4) if m else (4, rows // 4, cols)
    return [
        pltpu.VMEM((4, rows, cols), BF16),
        pltpu.VMEM((3, rows, cols), BF16),
        pltpu.VMEM((rows, cols), F32),
        pltpu.VMEM(part, BF16),
        pltpu.VMEM((3, *part[1:]), BF16),
        pltpu.VMEM(part, BF16),
    ]


def tail_kernel(nw, nt, last, a_t, wide_gu, by_gu, h, dy, far_wg, far_wu, far_down, by_h, out_d, *refs):
    step = pl.program_id(0)
    end = 2 * nw + nt - 1
    *refs, wg, wu, by_down, local = refs
    loads = [pltpu.make_async_copy(a, b, local.at[n]) for n, (a, b) in enumerate([(far_down, by_down), (far_wg, wg), (far_wu, wu)])]
    if last:
        out_g, out_u, term_g, term_u, *scratch = refs
        gate, up = Sum(1, term_g, *scratch[6:12], scratch[-2:]), Sum(2, term_u, *scratch[12:18], scratch[-2:])
    else:
        term_g, term_u, *scratch = refs
    down = Sum(0, by_down, *scratch[0:6], scratch[-2:])

    def begin():
        for load in loads:
            load.start()
        greet(all_peers())
        down.pair(far_down)

    def second():
        loads[0].wait()
        down.chips(far_down)

    def third():
        loads[1].wait()
        loads[2].wait()

    plan = [(0, begin), (1, second), (2 * nw, third), (nw + nw // 2, down.groups), (2 * nw, down.share), (2 * nw + 3, lambda: down.end(out_d))]
    if last:
        plan += [(nw, gate.pair), (nw + 1, gate.chips), (2 * nw + nt // 4, gate.groups), (2 * nw + nt // 2, gate.share)]
        plan += [(2 * nw, up.pair), (2 * nw + 1, up.chips), (end - 1, up.groups)]
    for n, f in plan:
        pl.when(step == n)(f)

    def weight(term, n):
        width = wide_gu.shape[2]
        got = dot(a_t[...], wide_gu[0]).astype(BF16)
        rows = term.shape[1]
        for s in range(8):
            term[s, :, pl.ds(pl.multiple_of(n * width, 128), width)] = got[s * rows : (s + 1) * rows]

    @pl.when(step < nw)
    def _():
        weight(term_g, step)

    @pl.when((step >= nw) & (step < 2 * nw))
    def _():
        weight(term_u, step - nw)

    @pl.when(step >= 2 * nw)
    def _():
        by_a = (dot(wg[...], by_gu[0], ((1,), (1,))) + dot(wu[...], by_gu[1], ((1,), (1,)))).T
        by_a = by_a.astype(BF16).astype(F32)
        wide = h[...].astype(F32)
        scale = lax.rsqrt(jnp.mean(wide * wide, -1, keepdims=True) + EPS)
        pull = jnp.mean(by_a * wide, -1, keepdims=True) * scale * scale * scale
        by_h[...] = (dy[...].astype(F32) + (by_a * scale - wide * pull).astype(BF16).astype(F32)).astype(BF16)

    if last:

        @pl.when(step == end)
        def _():
            up.share()
            gate.end(out_g)
            up.end(out_u)


def tail(a_t, by_gu, wg, wu, h, dy, by_down, last_layer, collective_id, width=512, tile=512):
    d, tokens = a_t.shape
    ff = wg.shape[1]
    nw, nt = ff // width, tokens // tile
    place = lambda i: jnp.maximum(i - 2 * nw, 0)
    rows = pl.BlockSpec((tile, d), lambda i: (place(i), 0))
    last = 2 * nw - 1
    gate_block, down_block = (d // 8, ff), (ff // 8, d)
    whole = lambda shape: pl.BlockSpec(shape, lambda i: (0,) * len(shape))
    blocks = [gate_block] * 2 if last_layer else [(8, *gate_block)] * 2
    scratch = sum_scratch(0, *down_block)
    if last_layer:
        scratch = [pltpu.VMEM((8, *gate_block), BF16)] * 2 + scratch + sum_scratch(1, *gate_block) + sum_scratch(2, *gate_block)
    return pl.pallas_call(
        functools.partial(tail_kernel, nw, nt, last_layer),
        grid=(2 * nw + nt,),
        out_shape=[
            jax.ShapeDtypeStruct((tokens, d), BF16),
            jax.ShapeDtypeStruct(down_block, BF16),
            *[jax.ShapeDtypeStruct(b, BF16) for b in blocks],
        ],
        in_specs=[
            constant(a_t.shape),
            pl.BlockSpec((1, tokens, width), lambda i: (jnp.minimum(i, last) // nw, 0, jnp.minimum(i, last) % nw)),
            pl.BlockSpec((2, tile, ff), lambda i: (0, place(i), 0)),
            rows,
            rows,
            *[pl.BlockSpec(memory_space=pl.ANY)] * 3,
        ],
        out_specs=[
            rows,
            whole(down_block),
            *[whole(b) for b in blocks],
        ],
        scratch_shapes=[
            *scratch,
            pltpu.SemaphoreType.DMA((3, 13)),
            pltpu.SemaphoreType.DMA((3, 13)),
            *[pltpu.VMEM(w.shape, BF16) for w in (wg, wu, by_down)],
            pltpu.SemaphoreType.DMA((3,)),
        ],
        compiler_params=pltpu.CompilerParams(
            collective_id=collective_id, has_side_effects=True, vmem_limit_bytes=VMEM_LIMIT, dimension_semantics=("arbitrary",)
        ),
        cost_estimate=pl.CostEstimate(flops=8 * tokens * d * ff, bytes_accessed=8 * tokens * ff, transcendentals=0),
        name="tail",
    )(a_t, by_gu, by_gu, h, dy, wg, wu, by_down)


def solution(mesh):
    def step(x, dy, *shards):
        layers = shards[0].shape[0]
        assert layers == 2
        h, weights = forward(x[0], shards, 1)
        inputs = [x[0], h]
        by_h, mine, terms = dy[0], [None] * layers, ()
        for n in reversed(range(layers)):
            by_gu, a_t, by_down, *summed = act(inputs[n], by_h, weights[n], terms, 2 * layers + n)
            if terms:
                mine[n + 1] = [*summed, mine[n + 1]]
            by_h, by_d, *terms = tail(a_t, by_gu, *weights[n][:2], inputs[n], by_h, by_down, n == 0, layers + n)
            mine[n] = by_d if n else [*terms, by_d]
        return (by_h[None], *(jnp.stack([mine[n][i] for n in range(layers)]) for i in range(3)))

    states, cut = P(("rep", "r", "s"), None, None), P(None, "s", None)
    return jax.shard_map(
        step,
        mesh=mesh,
        in_specs=(states, states) + (cut,) * 3,
        out_specs=(states,) + (P("rep", "s", None),) * 3,
        check_vma=False,
    )
```

```python
import functools

import jax
import jax.numpy as jnp
from jax import lax
from jax.experimental import pallas as pl
from jax.experimental.pallas import tpu as pltpu
from jax.sharding import PartitionSpec as P

F32, BF16 = jnp.float32, jnp.bfloat16
MESH = pl.DeviceIdType.MESH
VMEM_LIMIT = 66_000_000
EPS = 1e-6


def dot(a, b, dims=((1,), (0,))):
    return lax.dot_general(a, b, (dims, ((), ())), preferred_element_type=F32)


def places():
    me = lax.axis_index("s")
    core, y, x = me % 2, (me // 2) % 2, me // 4
    to_x, to_y = 4 - 8 * x, 2 - 4 * y
    return me, me + 1 - 2 * core, me + to_x, me + to_y, me + to_x + to_y


def all_peers():
    _, mate, *near = places()
    z = lax.axis_index("r")
    return [{"s": p} for p in (mate, *near)] + [{"r": (z + k) % 4} for k in (1, 2, 3)]


def hail(peers):
    barrier = pltpu.get_barrier_semaphore()
    for peer in peers:
        pl.semaphore_signal(barrier, inc=1, device_id=peer, device_id_type=MESH)


def hear(peers):
    pl.semaphore_wait(pltpu.get_barrier_semaphore(), len(peers))


def greet(peers):
    hail(peers)
    hear(peers)


def remote(src, dst, send, recv, peer):
    return pltpu.make_async_remote_copy(src_ref=src, dst_ref=dst, send_sem=send, recv_sem=recv, device_id=peer, device_id_type=MESH)


class Piece:
    def __init__(self, block, at, half, send, recv):
        self.me, self.mate, self.xn, self.yn, self.dn = places()
        self.block, self.at, self.half, self.send, self.recv = block, at, half, send, recv

    def copy(self, k):
        sems = self.send.at[k], self.recv.at[k]
        if k < 3:
            return remote(self.block, self.at(self.me), *sems, {"s": (self.mate, self.xn, self.yn)[k]})
        if k == 3:
            return remote(self.half(self.xn, 0), self.half(self.xn, 0), *sems, {"s": self.yn})
        if k == 4:
            return remote(self.half(self.yn, 1), self.half(self.yn, 1), *sems, {"s": self.xn})
        which = (self.xn, self.yn, self.dn)[k - 5]
        return remote(self.at(which), self.at(which), *sems, {"s": self.mate})

    def begin(self):
        for k in (1, 2, 0):
            self.copy(k).start()

    def forward(self):
        self.copy(1).wait_recv()
        self.copy(2).wait_recv()
        for k in (3, 4, 5, 6):
            self.copy(k).start()

    def relay(self):
        self.copy(3).wait_recv()
        self.copy(4).wait_recv()
        self.copy(7).start()

    def settle(self):
        for k in (0, 5, 6, 7):
            self.copy(k).wait_recv()

    def drain(self):
        for k in range(8):
            self.copy(k).wait_send()


def by_columns(block, whole, first, count, *sems):
    cut = lambda slot, start, n: whole.at[slot, :, pl.ds(start, n)]
    return Piece(
        block.at[0, :, pl.ds(first, count)],
        lambda slot: cut(slot, first, count),
        lambda slot, h: cut(slot, first + h * (count // 2), count // 2),
        *sems,
    )


def by_rows(block, whole, *sems):
    n = whole.shape[1] // 2
    return Piece(block.at[0], lambda slot: whole.at[slot], lambda slot, h: whole.at[slot, pl.ds(h * n, n), :], *sems)


def normed(h):
    wide = h.astype(F32)
    scale = lax.rsqrt(jnp.mean(wide * wide, -1, keepdims=True) + EPS)
    return wide, scale, (wide * scale).astype(BF16)


def forward_kernel(nt, nc, x, sg, su, sd, ng, nu, nd, out, og, ou, od, pg, pu, pd, wg, wu, wd, a, hidden, send, recv, local):
    step = pl.program_id(0)
    d, ff = wg.shape[0] * wg.shape[1], wg.shape[2]
    tile, chunk = x.shape[0], ff // nc
    me = lax.axis_index("s")
    sems = lambda n: (send.at[n], recv.at[n])
    c = [
        [by_columns(shard, whole, k * chunk, chunk, *sems(2 * k + n)) for n, (shard, whole) in enumerate([(sg, wg), (su, wu)])]
        for k in range(nc)
    ]
    down = [by_rows(sd, wd, *sems(2 * nc))]
    g1 = [by_columns(ng, pg, 0, ff, *sems(2 * nc + 1))]
    u1 = [by_columns(nu, pu, 0, ff, *sems(2 * nc + 2))]
    d1 = [by_rows(nd, pd, *sems(2 * nc + 3))]
    keep = [pltpu.make_async_copy(p.at[0], q.at[me], local.at[n]) for n, (p, q) in enumerate([(ng, pg), (nu, pu), (nd, pd)])]
    save = [pltpu.make_async_copy(p, q, local.at[3 + n]) for n, (p, q) in enumerate([(wg, og), (wu, ou), (wd, od)])]

    def do(*acts):
        for name, pieces in acts:
            for piece in pieces:
                getattr(piece, name)()

    def first():
        mate, xn, yn = places()[1:4]
        greet([{"s": p} for p in (mate, xn, yn)])
        do(("begin", c[0]), ("begin", c[1]))
        for shard, whole in ((sg, wg), (su, wu), (sd, wd)):
            whole[me] = shard[0]
        for copy in keep:
            copy.start()
        do(("forward", c[0]), ("begin", c[2]), ("relay", c[0]), ("settle", c[0]))

    def all_here():
        do(("settle", down))
        for copy in save:
            copy.start()

    plan = {
        0: first,
        1: lambda: do(("forward", c[1]), ("begin", c[3])),
        3: lambda: do(("relay", c[1]), ("forward", c[2]), ("begin", down)),
        4: lambda: do(("settle", c[1])),
        5: lambda: do(("forward", c[3]), ("begin", g1)),
        6: lambda: do(("relay", c[2])),
        8: lambda: do(("settle", c[2]), ("forward", down), ("begin", u1)),
        9: lambda: do(("relay", c[3])),
        12: lambda: do(("settle", c[3]), ("relay", down), ("forward", g1), ("begin", d1)),
        16: all_here,
        17: lambda: do(("forward", u1), ("relay", g1)),
        19: lambda: do(("forward", d1)),
    }
    for n, f in plan.items():
        pl.when(step == n)(f)

    @pl.when(step < nt)
    def _():
        a[step] = normed(x[...])[2]

    @pl.when(step < nt * nc)
    def _():
        cut = pl.ds(pl.multiple_of(step // nt * chunk, chunk), chunk)
        here = a[step % nt]
        gate = dot(here, wg[:, :, cut].reshape(d, chunk))
        up = dot(here, wu[:, :, cut].reshape(d, chunk))
        hidden[step % nt, :, cut] = (gate * lax.logistic(gate) * up).astype(BF16)

    @pl.when(step >= nt * nc)
    def _():
        below = dot(hidden[step - nt * nc], wd[...].reshape(ff, d)).astype(BF16)
        out[...] = (x[...].astype(F32) + below.astype(F32)).astype(BF16)

    @pl.when(step == nt * nc + nt - 1)
    def _():
        do(("relay", u1), ("relay", d1), ("settle", g1), ("settle", u1), ("settle", d1))
        for pieces in (*c, down, g1, u1, d1):
            do(("drain", pieces))
        for copy in (*keep, *save):
            copy.wait()


def constant(shape):
    return pl.BlockSpec(shape, lambda i: (0,) * len(shape), pipeline_mode=pl.Buffered(1))


def forward(x, shards, collective_id, nt=4, nc=4):
    tokens, d = x.shape
    ff = shards[0].shape[2]
    tile = tokens // nt
    wholes = [(8, *w.shape[1:]) for w in shards]
    spot = lambda i: jnp.where(i < nt, i, jnp.where(i < nt * nc, nt - 1, i - nt * nc))
    layer = lambda w, n: pl.BlockSpec((1, *w.shape[1:]), lambda i: (n, 0, 0), pipeline_mode=pl.Buffered(1))
    out, *got = pl.pallas_call(
        functools.partial(forward_kernel, nt, nc),
        grid=(nt * nc + nt,),
        out_shape=[jax.ShapeDtypeStruct(x.shape, BF16), *[jax.ShapeDtypeStruct(w, BF16) for w in wholes * 2]],
        in_specs=[pl.BlockSpec((tile, d), lambda i: (spot(i), 0)), *[layer(w, n) for n in range(2) for w in shards]],
        out_specs=[pl.BlockSpec((tile, d), lambda i: (jnp.maximum(i - nt * nc, 0), 0)), *[pl.BlockSpec(memory_space=pl.ANY)] * 6],
        scratch_shapes=[
            *[pltpu.VMEM(w, BF16) for w in wholes],
            pltpu.VMEM((nt, tile, d), BF16),
            pltpu.VMEM((nt, tile, ff), BF16),
            pltpu.SemaphoreType.DMA((2 * nc + 4, 8)),
            pltpu.SemaphoreType.DMA((2 * nc + 4, 8)),
            pltpu.SemaphoreType.DMA((6,)),
        ],
        compiler_params=pltpu.CompilerParams(
            collective_id=collective_id, has_side_effects=True, vmem_limit_bytes=VMEM_LIMIT, dimension_semantics=("arbitrary",)
        ),
        cost_estimate=pl.CostEstimate(flops=6 * tokens * d * ff, bytes_accessed=4 * tokens * d, transcendentals=0),
        name="forward",
    )(x, *shards, *shards)
    got = [w.reshape(-1, w.shape[-1]) for w in got]
    return out, [got[:3], got[3:]]


def act_kernel(steps, chunk, sums, h, dy, wg, wu, wd, *refs):
    step = pl.program_id(0)
    if sums:
        far_g, far_u, by_gu, a_t, by_down, out_g, out_u, total, *scratch, term_g, term_u, local = refs
        loads = [pltpu.make_async_copy(a, b, local.at[n]) for n, (a, b) in enumerate([(far_g, term_g), (far_u, term_u)])]
        gate_sum = Sum(1, term_g, *scratch[:6], scratch[-2:])
        up_sum = Sum(2, term_u, *scratch[6:12], scratch[-2:])

        def begin():
            for load in loads:
                load.start()
            greet(all_peers())
            gate_sum.pair(far_g)
            up_sum.pair(far_u)

        def second():
            for load in loads:
                load.wait()
            gate_sum.chips(far_g)
            up_sum.chips(far_u)

        plan = [(0, begin), (1, second), (3, gate_sum.groups), (5, gate_sum.share), (5, up_sum.groups), (7, up_sum.share)]
        for n, f in plan:
            pl.when(step == steps * n // 8)(f)
    else:
        by_gu, a_t, by_down, total = refs

    @pl.when(step == 0)
    def _():
        total[...] = jnp.zeros_like(total)

    _, _, a = normed(h[...])
    g = dy[...]
    a_t[...] = a.T
    g_t = g.T
    for j in range(wg.shape[1] // chunk):
        cut = pl.ds(j * chunk, chunk)
        gate, up = dot(a, wg[:, cut]), dot(a, wu[:, cut])
        by_hidden = dot(g, wd[cut, :], ((1,), (1,))).astype(BF16).astype(F32)
        share = lax.logistic(gate)
        silu = gate * share
        by_gu[0, :, cut] = (by_hidden * up * (share + silu * (1.0 - share))).astype(BF16)
        by_gu[1, :, cut] = (by_hidden * silu).astype(BF16)
        total[:, cut] += dot(g_t, (silu * up).astype(BF16))

    @pl.when(step == steps - 1)
    def _():
        n = by_down.shape[1]
        for s in range(by_down.shape[0]):
            by_down[s] = total[:, s * n : (s + 1) * n].T.astype(BF16)
        if sums:
            gate_sum.end(out_g)
            up_sum.end(out_u)


def act(h, dy, weights, terms=(), collective_id=None, tile=512, chunk=256):
    tokens, d = h.shape
    ff = weights[0].shape[1]
    steps = tokens // tile
    rows = pl.BlockSpec((tile, d), lambda i: (i, 0))
    block = (d // 8, ff)
    scratch, extra = [], {}
    if terms:
        scratch = [*sum_scratch(1, *block), *sum_scratch(2, *block), pltpu.SemaphoreType.DMA((3, 13)), pltpu.SemaphoreType.DMA((3, 13))]
        scratch += [pltpu.VMEM(w.shape, BF16) for w in terms] + [pltpu.SemaphoreType.DMA((2,))]
        extra = dict(collective_id=collective_id, has_side_effects=True)
    return pl.pallas_call(
        functools.partial(act_kernel, steps, chunk, bool(terms)),
        grid=(steps,),
        out_shape=[
            jax.ShapeDtypeStruct((2, tokens, ff), BF16),
            jax.ShapeDtypeStruct((d, tokens), BF16),
            jax.ShapeDtypeStruct((8, ff // 8, d), BF16),
            *[jax.ShapeDtypeStruct(block, BF16) for _ in terms],
        ],
        in_specs=[rows, rows, *[constant(w.shape) for w in weights], *[pl.BlockSpec(memory_space=pl.ANY) for _ in terms]],
        out_specs=[
            pl.BlockSpec((2, tile, ff), lambda i: (0, i, 0)),
            pl.BlockSpec((d, tile), lambda i: (0, i)),
            pl.BlockSpec((8, ff // 8, d), lambda i: (0, 0, 0)),
            *[pl.BlockSpec(block, lambda i: (0, 0)) for _ in terms],
        ],
        scratch_shapes=[pltpu.VMEM((d, ff), F32), *scratch],
        compiler_params=pltpu.CompilerParams(vmem_limit_bytes=VMEM_LIMIT, dimension_semantics=("arbitrary",), **extra),
        cost_estimate=pl.CostEstimate(flops=8 * tokens * d * ff, bytes_accessed=8 * tokens * ff, transcendentals=0),
        name="act",
    )(h, dy, *weights, *terms)


class Sum:
    def __init__(self, m, term, got0, got1, own, parts, got2, done, sems):
        self.m, self.term, self.got0, self.got1, self.own, self.parts, self.got2, self.done = m, term, got0, got1, own, parts, got2, done
        self.sems = sems
        self.me, self.mate, xn, yn, dn = places()
        self.near = (xn, yn, dn)
        self.z = lax.axis_index("r")
        self.core, self.chip = self.me % 2, self.me // 2

    def copy(self, k, term=None):
        sems = self.sems[0].at[self.m, k], self.sems[1].at[self.m, k]
        if k < 4:
            return remote((self.term if term is None else term).at[2 * k + 1 - self.core], self.got0.at[k], *sems, {"s": self.mate})
        if k < 7:
            to = self.near[k - 4]
            return remote(self.got0.at[to // 2], self.got1.at[k - 4], *sems, {"s": to})
        if k < 10:
            z = (self.z + k - 6) % 4
            return remote(self.parts.at[z], self.got2.at[k - 7], *sems, {"r": z})
        z = (self.z + k - 9) % 4
        return remote(self.done.at[self.z], self.done.at[self.z], *sems, {"r": z})

    def start(self, ks):
        for k in ks:
            self.copy(k).start()

    def wait(self, ks):
        for k in ks:
            self.copy(k).wait()

    def pair(self, term=None):
        for k in range(4):
            self.copy(k, term).start()

    def chips(self, term=None):
        for k in range(4):
            self.copy(k, term).wait()
        for k, to in enumerate(self.near):
            chip = to // 2
            self.got0[chip] = (self.term[2 * chip + self.core].astype(F32) + self.got0[chip].astype(F32)).astype(BF16)
            self.copy(4 + k).start()
        self.own[...] = self.term[self.me].astype(F32) + self.got0[self.chip].astype(F32)

    def groups(self):
        self.wait(range(4, 7))
        whole = self.own[...] + self.got1[0].astype(F32) + self.got1[1].astype(F32) + self.got1[2].astype(F32)
        self.own[...] = whole
        n = self.parts.shape
        for q in range(4):
            self.parts[q] = (whole[:, q * n[2] : (q + 1) * n[2]] if self.m else whole[q * n[1] : (q + 1) * n[1]]).astype(BF16)
        self.start(range(7, 10))

    def share(self):
        self.wait(range(7, 10))
        n = self.parts.shape
        if self.m:
            mine = self.own[:, pl.ds(pl.multiple_of(self.z * n[2], 128), n[2])]
        else:
            mine = self.own[pl.ds(pl.multiple_of(self.z * n[1], 8), n[1]), :]
        for k in range(3):
            mine = mine + self.got2[k].astype(F32)
        self.done[self.z] = mine.astype(BF16)
        self.start(range(10, 13))

    def end(self, out):
        self.wait(range(10, 13))
        n = self.parts.shape
        for q in range(4):
            if self.m:
                out[:, q * n[2] : (q + 1) * n[2]] = self.done[q]
            else:
                out[q * n[1] : (q + 1) * n[1], :] = self.done[q]


def sum_scratch(m, rows, cols):
    part = (4, rows, cols // 4) if m else (4, rows // 4, cols)
    return [
        pltpu.VMEM((4, rows, cols), BF16),
        pltpu.VMEM((3, rows, cols), BF16),
        pltpu.VMEM((rows, cols), F32),
        pltpu.VMEM(part, BF16),
        pltpu.VMEM((3, *part[1:]), BF16),
        pltpu.VMEM(part, BF16),
    ]


def tail_kernel(nw, nt, last, a_t, wide_gu, by_gu, h, dy, far_wg, far_wu, far_down, by_h, out_d, *refs):
    step = pl.program_id(0)
    end = 2 * nw + nt - 1
    *refs, wg, wu, by_down, local = refs
    loads = [pltpu.make_async_copy(a, b, local.at[n]) for n, (a, b) in enumerate([(far_down, by_down), (far_wg, wg), (far_wu, wu)])]
    if last:
        out_g, out_u, term_g, term_u, *scratch = refs
        gate, up = Sum(1, term_g, *scratch[6:12], scratch[-2:]), Sum(2, term_u, *scratch[12:18], scratch[-2:])
    else:
        term_g, term_u, *scratch = refs
    down = Sum(0, by_down, *scratch[0:6], scratch[-2:])

    def begin():
        for load in loads:
            load.start()
        hail(all_peers())

    def meet():
        hear(all_peers())
        down.pair(far_down)

    def second():
        loads[0].wait()
        down.chips(far_down)

    def third():
        loads[1].wait()
        loads[2].wait()

    plan = [(0, begin), (1, meet), (2, second), (2 * nw, third)]
    plan += [(2 * nw - 1, down.groups), (2 * nw + 1, down.share), (end - 3, lambda: down.end(out_d))]
    if last:
        plan += [(nw, gate.pair), (nw + 1, gate.chips), (2 * nw + 2, gate.groups), (2 * nw + 4, gate.share)]
        plan += [(2 * nw, up.pair), (2 * nw + 1, up.chips), (end - 1, up.groups)]
    for n, f in plan:
        pl.when(step == n)(f)

    def weight(term, n):
        width = wide_gu.shape[2]
        got = dot(a_t[...], wide_gu[0]).astype(BF16)
        rows = term.shape[1]
        for s in range(8):
            term[s, :, pl.ds(pl.multiple_of(n * width, 128), width)] = got[s * rows : (s + 1) * rows]

    @pl.when(step < nw)
    def _():
        weight(term_g, step)

    @pl.when((step >= nw) & (step < 2 * nw))
    def _():
        weight(term_u, step - nw)

    @pl.when(step >= 2 * nw)
    def _():
        by_a = (dot(wg[...], by_gu[0], ((1,), (1,))) + dot(wu[...], by_gu[1], ((1,), (1,)))).T
        by_a = by_a.astype(BF16).astype(F32)
        wide = h[...].astype(F32)
        scale = lax.rsqrt(jnp.mean(wide * wide, -1, keepdims=True) + EPS)
        pull = jnp.mean(by_a * wide, -1, keepdims=True) * scale * scale * scale
        by_h[...] = (dy[...].astype(F32) + (by_a * scale - wide * pull).astype(BF16).astype(F32)).astype(BF16)

    if last:

        @pl.when(step == end)
        def _():
            up.share()
            gate.end(out_g)
            up.end(out_u)


def tail(a_t, by_gu, wg, wu, h, dy, by_down, last_layer, collective_id, width=512, tile=512):
    d, tokens = a_t.shape
    ff = wg.shape[1]
    nw, nt = ff // width, tokens // tile
    place = lambda i: jnp.maximum(i - 2 * nw, 0)
    rows = pl.BlockSpec((tile, d), lambda i: (place(i), 0))
    last = 2 * nw - 1
    gate_block, down_block = (d // 8, ff), (ff // 8, d)
    whole = lambda shape: pl.BlockSpec(shape, lambda i: (0,) * len(shape))
    blocks = [gate_block] * 2 if last_layer else [(8, *gate_block)] * 2
    scratch = sum_scratch(0, *down_block)
    if last_layer:
        scratch = [pltpu.VMEM((8, *gate_block), BF16)] * 2 + scratch + sum_scratch(1, *gate_block) + sum_scratch(2, *gate_block)
    return pl.pallas_call(
        functools.partial(tail_kernel, nw, nt, last_layer),
        grid=(2 * nw + nt,),
        out_shape=[
            jax.ShapeDtypeStruct((tokens, d), BF16),
            jax.ShapeDtypeStruct(down_block, BF16),
            *[jax.ShapeDtypeStruct(b, BF16) for b in blocks],
        ],
        in_specs=[
            constant(a_t.shape),
            pl.BlockSpec((1, tokens, width), lambda i: (jnp.minimum(i, last) // nw, 0, jnp.minimum(i, last) % nw)),
            pl.BlockSpec((2, tile, ff), lambda i: (0, place(i), 0)),
            rows,
            rows,
            *[pl.BlockSpec(memory_space=pl.ANY)] * 3,
        ],
        out_specs=[
            rows,
            whole(down_block),
            *[whole(b) for b in blocks],
        ],
        scratch_shapes=[
            *scratch,
            pltpu.SemaphoreType.DMA((3, 13)),
            pltpu.SemaphoreType.DMA((3, 13)),
            *[pltpu.VMEM(w.shape, BF16) for w in (wg, wu, by_down)],
            pltpu.SemaphoreType.DMA((3,)),
        ],
        compiler_params=pltpu.CompilerParams(
            collective_id=collective_id, has_side_effects=True, vmem_limit_bytes=VMEM_LIMIT, dimension_semantics=("arbitrary",)
        ),
        cost_estimate=pl.CostEstimate(flops=8 * tokens * d * ff, bytes_accessed=8 * tokens * ff, transcendentals=0),
        name="tail",
    )(a_t, by_gu, by_gu, h, dy, wg, wu, by_down)


def solution(mesh):
    def step(x, dy, *shards):
        layers = shards[0].shape[0]
        assert layers == 2
        h, weights = forward(x[0], shards, 1)
        inputs = [x[0], h]
        by_h, mine, terms = dy[0], [None] * layers, ()
        for n in reversed(range(layers)):
            by_gu, a_t, by_down, *summed = act(inputs[n], by_h, weights[n], terms, 2 * layers + n)
            if terms:
                mine[n + 1] = [*summed, mine[n + 1]]
            by_h, by_d, *terms = tail(a_t, by_gu, *weights[n][:2], inputs[n], by_h, by_down, n == 0, layers + n)
            mine[n] = by_d if n else [*terms, by_d]
        return (by_h[None], *(jnp.stack([mine[n][i] for n in range(layers)]) for i in range(3)))

    states, cut = P(("rep", "r", "s"), None, None), P(None, "s", None)
    return jax.shard_map(
        step,
        mesh=mesh,
        in_specs=(states, states) + (cut,) * 3,
        out_specs=(states,) + (P("rep", "s", None),) * 3,
        check_vma=False,
    )
```
